32 devices in a mesh: tok: 16 (over z, y, core), col: 2 (over x).
Axes of the slice: x: 2, y: 2, z: 4, core: 2. Of those that a mesh axis runs over, the one named last changes fastest.
Arguments:
- hidden: bfloat16 [4096, 8192], P('tok'), may hold values from -6 to 6
- norm_gain: float32 [8192], replicated, may hold values from 0.1 to 1.9
- token_ids: int32 [4096], P('tok'), may hold values from 0 to 128000, as said below
- owner: int32 [1], replicated, may hold values from 0 to 15
- query_store: bfloat16 [16, 8192, 4096], P('tok', None, 'col'), may hold values from -0.0625 to 0.0625
- key_store: bfloat16 [16, 8192, 512], P('tok', None, 'col'), may hold values from -0.0625 to 0.0625
Outputs:
- queries: bfloat16 [4096, 4096], P('tok', 'col')
- keys: bfloat16 [4096, 512], P('tok', 'col')
- hessian: float32 [8192, 8192], P('col', 'tok')
The draws below stay inside these ranges and needn't reach their ends.
Inputs may be any that keep to these rules, and one draw needn't show every extreme that they name: `token_ids`: id 128000 marks the first token of a document; every other id is below it.
All inputs are finite; a program needn't handle non-finite values.
Results may differ from the reference program's by a relative error of at most 0.0049.
Values may be sent and summed in bfloat16 or wider, within the bound.
A program may use at most 256 MiB of HBM per device.

```python
import jax
import jax.numpy as jnp
from jax import lax

D = 8192
HEAD = 128
SEQ = 128
QCOLS = 4096
KCOLS = 512
TOKENS = 4096
LAYERS = 16
N_TOK = 16


def draw_token_ids(key, part):
    base = jax.random.fold_in(key, 11)
    first_key, second_key = jax.random.split(base)
    marks = jax.random.randint(first_key, (TOKENS,), 0, 32) == 0
    words = jax.random.randint(second_key, (TOKENS,), 0, 128000)
    return jnp.where(marks, 128000, words).astype(jnp.int32)


def block_levels(rng, shape, shards, least, high):
    loudness, own = 1.0, jax.random.fold_in(rng, 6)
    for axis_at, blocks in shards:
        heights = jnp.exp(jax.random.uniform(jax.random.fold_in(own, axis_at), (blocks,), jnp.float32, least / len(shards), high / len(shards)))
        loudness = loudness * jnp.repeat(heights, shape[axis_at] // blocks).reshape([-1 if axis == axis_at else 1 for axis in range(len(shape))])
    return loudness


def normal_values(stream_key, extent, scale, reach, cuts=(), kind=jnp.bfloat16):
    array = scale * jax.random.normal(stream_key, extent, jnp.float32)
    if cuts:
        array = array * block_levels(stream_key, extent, cuts, -0.22, 0.18)
    return jnp.clip(array, -reach, reach).astype(kind)


def setup_inputs(seed: int = 0) -> dict:
    splits = jax.random.split(jax.random.key(seed), 7)
    return {
        "hidden": normal_values(splits[0], (TOKENS, D), 1.0, 6.0, ((0, 16),)),
        "norm_gain": jnp.clip(1.0 + 0.18 * jax.random.normal(splits[1], (D,), jnp.float32), 0.1, 1.9),
        "token_ids": draw_token_ids(jax.random.fold_in(splits[6], 71), 0),
        "owner": jax.random.randint(splits[3], (1,), 0, N_TOK).astype(jnp.int32),
        "query_store": normal_values(splits[4], (LAYERS, D, QCOLS), D ** -0.5, 0.0625, ((0, 16), (2, 2))),
        "key_store": normal_values(splits[5], (LAYERS, D, KCOLS), D ** -0.5, 0.0625, ((0, 16), (2, 2))),
    }


begin_token = 128000
rope_base = 500000.0

def positions(token_ids):
    samples = token_ids.reshape(-1, SEQ)
    index = jnp.arange(SEQ, dtype=jnp.int32)
    starts = jnp.where(samples == begin_token, index[None, :], jnp.zeros_like(samples))
    latest = lax.cummax(starts, axis=1)
    return (index[None, :] - latest).reshape(-1)

def rotate(values, place, start):
    width = values.shape[1]
    dims = (start + jnp.arange(width, dtype=jnp.int32)) % HEAD
    pair = (dims[0::2] // 2).astype(jnp.float32)
    freq = jnp.power(jnp.float32(rope_base), -2.0 * pair / HEAD)
    angle = place.astype(jnp.float32)[:, None] * freq[None, :]
    cosine = jnp.cos(angle)
    sine = jnp.sin(angle)
    even = values[:, 0::2]
    odd = values[:, 1::2]
    first = even * cosine - odd * sine
    second = even * sine + odd * cosine
    return jnp.stack([first, second], axis=-1).reshape(values.shape[0], width)

def normalize(hidden, norm_gain):
    wide = hidden.astype(jnp.float32)
    meansq = lax.optimization_barrier(jnp.mean(wide * wide, axis=-1, keepdims=True))
    return (wide * lax.rsqrt(meansq + 1e-05) * norm_gain[None, :]).astype(jnp.bfloat16)

def reference(hidden, norm_gain, token_ids, owner, query_store, key_store):
    normed = normalize(hidden, norm_gain)
    place = positions(token_ids)
    slot = owner[0].astype(jnp.int32)
    weight_q = lax.dynamic_index_in_dim(query_store, slot, 0, keepdims=False)
    weight_k = lax.dynamic_index_in_dim(key_store, slot, 0, keepdims=False)
    raw_q = jnp.dot(normed, weight_q, preferred_element_type=jnp.float32)
    raw_k = jnp.dot(normed, weight_k, preferred_element_type=jnp.float32)
    queries = rotate(raw_q, place, 0).astype(jnp.bfloat16)
    keys = rotate(raw_k, place, 0).astype(jnp.bfloat16)
    gram = lax.dot_general(normed, normed, (((0,), (0,)), ((), ())), preferred_element_type=jnp.float32)
    hessian = gram * (2.0 / TOKENS)
    return (queries, keys, hessian)
```

```python
import jax
import jax.numpy as jnp
from jax import lax
from jax.sharding import PartitionSpec as P

HEAD = 128
SEQ = 128


begin_token = 128000
rope_base = 500000.0


def scatter_weights(query, key, owner):
    groups = lax.axis_size("tok")
    depth, width = query.shape
    piece = width // groups
    mine = lax.axis_index("tok") == owner
    query = jnp.moveaxis(query.reshape(depth, groups, piece), 1, 0)
    key = key.reshape(groups, depth * key.shape[1] // groups // piece, piece)
    both = jnp.concatenate([query, key], axis=1)
    return jnp.where(mine, both, jnp.zeros_like(both))


def positions(token_ids):
    samples = token_ids.reshape(-1, SEQ)
    index = jnp.arange(SEQ, dtype=jnp.int32)
    starts = jnp.where(samples == begin_token, index[None, :], jnp.zeros_like(samples))
    latest = lax.cummax(starts, axis=1)
    return (index[None, :] - latest).reshape(-1)


def rotate(values, place, start):
    width = values.shape[1]
    period = HEAD if width % HEAD == 0 else width
    dims = (start + jnp.arange(period, dtype=jnp.int32)) % HEAD
    pair = (dims // 2).astype(jnp.float32)
    freq = jnp.power(jnp.float32(rope_base), -2.0 * pair / HEAD)
    angle = place.astype(jnp.float32)[:, None] * freq[None, :]
    even = dims % 2 == 0
    sine = jnp.where(even[None, :], -jnp.sin(angle), jnp.sin(angle))
    cosine, sine = lax.optimization_barrier((jnp.cos(angle), sine))
    cosine = jnp.tile(cosine, (1, width // period))
    sine = jnp.tile(sine, (1, width // period))
    following = jnp.concatenate([values[:, 1:], values[:, :1]], axis=1)
    previous = jnp.concatenate([values[:, -1:], values[:, :-1]], axis=1)
    even = jnp.arange(width, dtype=jnp.int32) % 2 == 0
    other = jnp.where(even[None, :], following, previous)
    return values * cosine + other * sine


def normalize(hidden, norm_gain):
    wide = hidden.astype(jnp.float32)
    meansq = jnp.mean(wide * wide, axis=-1, keepdims=True)
    return (wide * lax.rsqrt(meansq + 1e-05) * norm_gain[None, :]).astype(jnp.bfloat16)


def transposed_product(left, right):
    return lax.dot_general(
        left, right, (((0,), (0,)), ((), ())), preferred_element_type=jnp.float32
    )


def shards(hidden, norm_gain, token_ids, owner, query_store, key_store):
    normed = normalize(hidden, norm_gain)
    place = positions(token_ids)
    column = lax.axis_index("col")
    row_width = normed.shape[1] // lax.axis_size("col")
    row_block = lax.dynamic_slice_in_dim(normed, column * row_width, row_width, 1)
    total_tokens = normed.shape[0] * lax.axis_size("tok")
    groups, parts = lax.axis_size("tok"), lax.axis_size("col")
    depth, q_width = query_store.shape[1:]
    k_width = key_store.shape[2]
    masked = scatter_weights(query_store[0], key_store[0], owner[0])
    gathered = lax.all_gather(row_block, "tok", axis=0, tiled=True)
    col_block = lax.all_to_all(normed, "tok", split_axis=1, concat_axis=0, tiled=True)
    masked, gathered = lax.optimization_barrier((masked, gathered))
    owned = lax.psum_scatter(masked, "tok", scatter_dimension=0, tiled=False)
    gram = transposed_product(gathered, col_block)
    hessian = gram * (2.0 / total_tokens)
    key_rows = owned[depth:].reshape(depth // groups, k_width)
    weight_k = lax.all_gather(key_rows, "tok", axis=0, tiled=True)
    weight_q = lax.all_to_all(owned[:depth], "col", split_axis=0, concat_axis=1, tiled=True)
    partial = jnp.dot(gathered, weight_q, preferred_element_type=jnp.float32).astype(jnp.bfloat16)
    partial = lax.all_to_all(partial, "col", split_axis=1, concat_axis=0, tiled=True)
    partial = partial.reshape(parts, total_tokens, q_width // groups).astype(jnp.float32)
    summed = jnp.sum(partial, axis=0).astype(jnp.bfloat16)
    raw_q = lax.all_to_all(summed, "tok", split_axis=0, concat_axis=1, tiled=True).astype(jnp.float32)
    raw_k = jnp.dot(normed, weight_k, preferred_element_type=jnp.float32)
    queries = rotate(raw_q, place, column * q_width).astype(jnp.bfloat16)
    keys = rotate(raw_k, place, column * k_width).astype(jnp.bfloat16)
    return (queries, keys, hessian)


def solution(mesh):
    placed = (P("tok", None), P(), P("tok"), P(), P("tok", None, "col"), P("tok", None, "col"))
    return jax.shard_map(
        shards,
        mesh=mesh,
        in_specs=placed,
        out_specs=(P("tok", "col"), P("tok", "col"), P("col", "tok")),
        check_vma=False,
    )
```
